32 devices in a mesh: dp: 8 (over y, x, core), tensor: 4 (over z).
Axes of the slice: x: 2, y: 2, z: 4, core: 2. Of those that a mesh axis runs over, the one named last changes fastest.
Arguments:
- text: bfloat16 [8, 256, 5120], P('dp', None, 'tensor'), may hold values from -6 to 6
- prompts: bfloat16 [8, 100, 5120], P('dp', None, 'tensor'), may hold values from -6 to 6
- gain: float32 [5120], replicated, may hold values from 0.1 to 1.9
- w_query: bfloat16 [5120, 3072], P(None, 'tensor'), may hold values from -0.069877124 to 0.069877124, as said below
- w_key: bfloat16 [5120, 3072], P(None, 'tensor'), may hold values from -1.2577882 to 1.2577882, as said below
- w_value: bfloat16 [5120, 3072], P(None, 'tensor'), may hold values from -0.078125 to 0.078125
- cotangent: bfloat16 [8, 356, 3072], P('dp', None, 'tensor'), may hold values from -6 to 6
- task_of: int32 [8], replicated, may hold values from 0 to 7, as said below
- lengths: int32 [8], replicated, may hold values from 1 to 256, as said below
- slot: int32 [8], replicated, may hold values from 0 to 7, as said below
Outputs:
- attn_out: bfloat16 [8, 356, 3072], P('dp', None, 'tensor')
- prompt_grad: float32 [8, 100, 5120], P('dp', None, 'tensor')
The draws below stay inside these ranges and needn't reach their ends.
Inputs may be any that keep to these rules, and one draw needn't show every extreme that they name: `task_of`: nondecreasing along the source order. `lengths`: some example has exactly 256 text tokens; rows of an example beyond its length are padding. `slot`: a permutation of 0 to 7; position s lies on index s // 1 of dp. `w_query`: entries of order 5120 ** -0.5. `w_key`: entries of order 5120 ** -0.5 or larger.
All inputs are finite; a program needn't handle non-finite values.
Results may differ from the reference program's by a relative error of at most 0.0082.
Values may be sent and summed in bfloat16 or wider, within the bound.
A program may use at most 128 MiB of HBM per device.

```python
import math
import jax
import jax.numpy as jnp
from jax import lax

D = 5120
HEADS = 24
HD = 128
P_SIZE = 100
SEQ = 256
EX_DEV = 1
ROWS = 356
EXAMPLES = 8
TASKS = 8


def weight_base(key):
    return jax.random.truncated_normal(jax.random.fold_in(key, 11), -4.0, 4.0, (D, HEADS * HD), jnp.float32) / math.sqrt(D)


def draw_w_query(key, part):
    return weight_base(key).astype(jnp.bfloat16)


def draw_w_key(key, part):
    noise_part = jax.random.truncated_normal(jax.random.fold_in(key, 12), -4.0, 4.0, (D, HEADS * HD), jnp.float32) / math.sqrt(D)
    result = noise_part
    return result.astype(jnp.bfloat16)


def draw_task_of(key, part):
    first_key, second_key, third_key = jax.random.split(jax.random.fold_in(key, 21), 3)
    first_pick = jax.random.randint(first_key, (EXAMPLES,), 0, TASKS)
    second_pick = jax.random.randint(second_key, (EXAMPLES,), 0, TASKS)
    ranked = jnp.minimum(first_pick, second_pick)
    shuffle = jax.random.permutation(third_key, TASKS)
    return jnp.sort(shuffle[ranked]).astype(jnp.int32)


def length_base(key):
    first_key, second_key = jax.random.split(jax.random.fold_in(key, 31))
    raw_lengths = jax.random.randint(first_key, (EXAMPLES,), 1, SEQ + 1)
    longest = jax.random.randint(second_key, (), 0, EXAMPLES)
    return jnp.where(jnp.arange(EXAMPLES) == longest, SEQ, raw_lengths).astype(jnp.int32)


def draw_lengths(key, part):
    return length_base(key)


def draw_slot(key, part):
    length_all = length_base(key)
    device_count = EXAMPLES // EX_DEV
    order = jnp.argsort(-length_all, stable=True)
    ranks = jnp.arange(EXAMPLES, dtype=jnp.int32)
    rounds = ranks // device_count
    column = ranks % device_count
    device = jnp.where(rounds % 2 == 0, column, device_count - 1 - column)
    placed = (device * EX_DEV + rounds).astype(jnp.int32)
    return jnp.zeros((EXAMPLES,), jnp.int32).at[order].set(placed)


def block_scale(key, dims, shards, least, largest):
    level, own = 1.0, jax.random.fold_in(key, 6)
    for dim, shards_of in shards:
        draws = jnp.exp(jax.random.uniform(jax.random.fold_in(own, dim), (shards_of,), jnp.float32, least / len(shards), largest / len(shards)))
        level = level * jnp.repeat(draws, dims[dim] // shards_of).reshape([-1 if axis == dim else 1 for axis in range(len(dims))])
    return level


def scatter_about(stream_key, shape, width, most, cuts=(), held_as=jnp.bfloat16):
    factor_of = block_scale(stream_key, shape, cuts, -0.22, 0.18) if cuts else 1.0
    array = jax.random.normal(stream_key, shape, jnp.float32) * width * factor_of
    return jnp.minimum(jnp.maximum(array, -most), most).astype(held_as)


def setup_inputs(seed: int = 0) -> dict:
    keys = jax.random.split(jax.random.key(seed), 11)
    return {
        "text": scatter_about(keys[0], (EXAMPLES, SEQ, D), 1.0, 6.0, ((0, 8), (2, 4))),
        "prompts": scatter_about(keys[1], (TASKS, P_SIZE, D), 1.0, 6.0, ((0, 8), (2, 4))),
        "gain": jnp.clip(1.0 + 0.18 * jax.random.normal(keys[2], (D,), jnp.float32), 0.1, 1.9),
        "w_query": draw_w_query(jax.random.fold_in(keys[10], 71), 0),
        "w_key": draw_w_key(jax.random.fold_in(keys[10], 71), 0),
        "w_value": scatter_about(keys[5], (D, HEADS * HD), D ** -0.5, 0.078125, ((1, 4),)),
        "cotangent": scatter_about(keys[6], (EXAMPLES, ROWS, HEADS * HD), 1.0, 6.0, ((0, 8), (2, 4))),
        "task_of": draw_task_of(jax.random.fold_in(keys[10], 71), 0),
        "lengths": draw_lengths(jax.random.fold_in(keys[10], 71), 0),
        "slot": draw_slot(jax.random.fold_in(keys[10], 71), 0),
    }


def rope_tables(row_count):
    half_dim = HD // 2
    frequency = 10000.0 ** (-jnp.arange(half_dim, dtype=jnp.float32) / half_dim)
    angle_table = jnp.arange(row_count, dtype=jnp.float32)[:, None] * frequency[None, :]
    return (jnp.cos(angle_table), jnp.sin(angle_table))

def rotate(vectors, cosine_table, sine_table):
    half_dim = vectors.shape[-1] // 2
    first_half = vectors[..., :half_dim]
    second_half = vectors[..., half_dim:]
    cosine_b = cosine_table[:, None, :]
    sine_b = sine_table[:, None, :]
    return jnp.concatenate([first_half * cosine_b - second_half * sine_b, second_half * cosine_b + first_half * sine_b], axis=-1)

def unrotate(vectors, cosine_table, sine_table):
    half_dim = vectors.shape[-1] // 2
    first_half = vectors[..., :half_dim]
    second_half = vectors[..., half_dim:]
    cosine_b = cosine_table[:, None, :]
    sine_b = sine_table[:, None, :]
    return jnp.concatenate([first_half * cosine_b + second_half * sine_b, second_half * cosine_b - first_half * sine_b], axis=-1)

def transpose_product(grad_low, matrix):
    return lax.dot_general(grad_low, matrix, (((1,), (1,)), ((), ())), preferred_element_type=jnp.float32)

def attention_window(full_rows, gain, w_query, w_key, w_value, cotangent, valid_rows, prompt_len):
    batch_size, row_count, model_width = full_rows.shape
    head_count = w_query.shape[1] // HD
    wide_rows = full_rows.astype(jnp.float32)
    inv_rms = lax.rsqrt(lax.optimization_barrier(jnp.mean(wide_rows * wide_rows, axis=-1)) + 1e-05)
    normed = (wide_rows * inv_rms[..., None] * gain).astype(jnp.bfloat16).reshape(batch_size * row_count, model_width)
    cosine_table, sine_table = rope_tables(row_count)

    def project(matrix):
        return jnp.dot(normed, matrix, preferred_element_type=jnp.float32).reshape(batch_size, row_count, head_count, HD)
    queries = rotate(project(w_query), cosine_table, sine_table).astype(jnp.bfloat16)
    key_rows = rotate(project(w_key), cosine_table, sine_table).astype(jnp.bfloat16)
    value_rows = project(w_value).astype(jnp.bfloat16)
    score_scale = 1.0 / math.sqrt(HD)
    scores = jnp.einsum('erhd,ekhd->ehrk', queries.astype(jnp.float32), key_rows.astype(jnp.float32)) * score_scale
    rows_at = jnp.arange(row_count, dtype=jnp.int32)
    row_limit = (prompt_len + valid_rows).astype(jnp.int32)
    allowed = (rows_at[None, None, :] <= rows_at[None, :, None]) & (rows_at[None, None, :] < row_limit[:, None, None])
    allowed = allowed[:, None]
    scores = jnp.where(allowed, scores, -1e+30)
    row_peak = lax.optimization_barrier(jnp.max(scores, axis=-1, keepdims=True))
    weights = jnp.where(allowed, jnp.exp(scores - row_peak), 0.0)
    probability = weights / lax.optimization_barrier(jnp.sum(weights, axis=-1, keepdims=True))
    probs_low = probability.astype(jnp.bfloat16)
    live_rows = rows_at[None, :] < row_limit[:, None]
    mixed_rows = jnp.einsum('ehrk,ekhd->erhd', probs_low.astype(jnp.float32), value_rows.astype(jnp.float32))
    mixed_rows = jnp.where(live_rows[:, :, None, None], mixed_rows, 0.0)
    output = mixed_rows.reshape(batch_size, row_count, head_count * HD).astype(jnp.bfloat16)
    upstream = jnp.where(live_rows[:, :, None, None], cotangent.reshape(batch_size, row_count, head_count, HD), 0.0).astype(jnp.bfloat16)
    grad_prob = jnp.einsum('erhd,ekhd->ehrk', upstream.astype(jnp.float32), value_rows.astype(jnp.float32))
    row_delta = lax.optimization_barrier(jnp.sum(probability * grad_prob, axis=-1, keepdims=True))
    grad_score = (probability * (grad_prob - row_delta)).astype(jnp.bfloat16)
    grad_query = jnp.einsum('ehrk,ekhd->erhd', grad_score[:, :, :prompt_len, :].astype(jnp.float32), key_rows.astype(jnp.float32)) * score_scale
    grad_key = jnp.einsum('ehrk,erhd->ekhd', grad_score[:, :, :, :prompt_len].astype(jnp.float32), queries.astype(jnp.float32)) * score_scale
    grad_value = jnp.einsum('ehrk,erhd->ekhd', probs_low[:, :, :, :prompt_len].astype(jnp.float32), upstream.astype(jnp.float32))
    cosine_lead = cosine_table[:prompt_len]
    sine_lead = sine_table[:prompt_len]
    flat_rows = batch_size * prompt_len
    grad_query = unrotate(grad_query, cosine_lead, sine_lead).astype(jnp.bfloat16).reshape(flat_rows, head_count * HD)
    grad_key = unrotate(grad_key, cosine_lead, sine_lead).astype(jnp.bfloat16).reshape(flat_rows, head_count * HD)
    grad_value = grad_value.astype(jnp.bfloat16).reshape(flat_rows, head_count * HD)
    grad_normed = transpose_product(grad_query, w_query) + transpose_product(grad_key, w_key) + transpose_product(grad_value, w_value)
    grad_normed = grad_normed.reshape(batch_size, prompt_len, model_width) * gain
    prompt_rows = wide_rows[:, :prompt_len]
    prompt_inv = inv_rms[:, :prompt_len, None]
    grad_rows = prompt_inv * grad_normed - prompt_rows * prompt_inv ** 3 * lax.optimization_barrier(jnp.mean(grad_normed * prompt_rows, axis=-1, keepdims=True))
    return (output, grad_rows)

def reference(text, prompts, gain, w_query, w_key, w_value, cotangent, task_of, lengths, slot):
    example_count = text.shape[0]
    positions = jnp.arange(example_count, dtype=jnp.int32)

    def one_slot(task_grads, place_id):
        hit_mask = slot == place_id
        source = jnp.sum(jnp.where(hit_mask, positions, 0)).astype(jnp.int32)
        task_id = jnp.sum(jnp.where(hit_mask, task_of, 0)).astype(jnp.int32)
        length = jnp.sum(jnp.where(hit_mask, lengths, 0)).astype(jnp.int32)
        joined = jnp.concatenate([prompts[task_id], text[source]], axis=0)[None]
        output, grad_rows = attention_window(joined, gain, w_query, w_key, w_value, cotangent[place_id][None], length[None], P_SIZE)
        task_grads = task_grads.at[task_id].add(grad_rows[0])
        return (task_grads, output[0])
    prompt_grad, attn_out = lax.scan(one_slot, jnp.zeros((TASKS, P_SIZE, D), jnp.float32), positions)
    return (attn_out, prompt_grad)
```

```python
import functools
import math

import jax
import jax.numpy as jnp
from jax import lax
from jax.experimental import pallas as pl
from jax.experimental.pallas import tpu as pltpu
from jax.sharding import PartitionSpec as P

HD = 128


def rope_tables(row_count):
    half_dim = HD // 2
    frequency = 10000.0 ** (-jnp.arange(half_dim, dtype=jnp.float32) / half_dim)
    angle_table = jnp.arange(row_count, dtype=jnp.float32)[:, None] * frequency[None, :]
    return (jnp.cos(angle_table), jnp.sin(angle_table))


def rotate(vectors, cosine_table, sine_table):
    half_dim = vectors.shape[-1] // 2
    first_half = vectors[..., :half_dim]
    second_half = vectors[..., half_dim:]
    cosine_b = cosine_table[:, None, :]
    sine_b = sine_table[:, None, :]
    return jnp.concatenate(
        [
            first_half * cosine_b - second_half * sine_b,
            second_half * cosine_b + first_half * sine_b,
        ],
        axis=-1,
    )


def unrotate(vectors, cosine_table, sine_table):
    half_dim = vectors.shape[-1] // 2
    first_half = vectors[..., :half_dim]
    second_half = vectors[..., half_dim:]
    cosine_b = cosine_table[:, None, :]
    sine_b = sine_table[:, None, :]
    return jnp.concatenate(
        [
            first_half * cosine_b + second_half * sine_b,
            second_half * cosine_b - first_half * sine_b,
        ],
        axis=-1,
    )


def transpose_product(grad_low, matrix):
    return lax.dot_general(
        grad_low, matrix, (((1,), (1,)), ((), ())), preferred_element_type=jnp.float32
    )


def attention_window(full_rows, gain, w_query, w_key, w_value, cotangent, valid_rows, prompt_len):
    batch_size, row_count, model_width = full_rows.shape
    head_count = w_query.shape[1] // HD
    wide_rows = full_rows.astype(jnp.float32)
    inv_rms = lax.rsqrt(jnp.mean(wide_rows * wide_rows, axis=-1) + 1e-05)
    normed = (
        (wide_rows * inv_rms[..., None] * gain)
        .astype(jnp.bfloat16)
        .reshape(batch_size * row_count, model_width)
    )
    cosine_table, sine_table = rope_tables(row_count)

    def project(matrix):
        return jnp.dot(normed, matrix, preferred_element_type=jnp.float32).reshape(
            batch_size, row_count, head_count, HD
        )

    queries = rotate(project(w_query), cosine_table, sine_table).astype(jnp.bfloat16)
    key_rows = rotate(project(w_key), cosine_table, sine_table).astype(jnp.bfloat16)
    value_rows = project(w_value).astype(jnp.bfloat16)
    score_scale = 1.0 / math.sqrt(HD)
    scores = (
        jnp.einsum("erhd,ekhd->ehrk", queries, key_rows, preferred_element_type=jnp.float32)
        * score_scale
    )
    rows_at = jnp.arange(row_count, dtype=jnp.int32)
    row_limit = prompt_len + valid_rows
    allowed = (rows_at[None, None, :] <= rows_at[None, :, None]) & (
        rows_at[None, None, :] < row_limit[:, None, None]
    )
    allowed = allowed[:, None]
    scores = jnp.where(allowed, scores, -1e30)
    row_peak = jnp.max(scores, axis=-1, keepdims=True)
    weights = jnp.where(allowed, jnp.exp(scores - row_peak), 0.0)
    probability = weights / jnp.sum(weights, axis=-1, keepdims=True)
    probs_low = probability.astype(jnp.bfloat16)
    live_rows = rows_at[None, :] < row_limit[:, None]
    mixed_rows = jnp.einsum(
        "ehrk,ekhd->erhd", probs_low, value_rows, preferred_element_type=jnp.float32
    )
    mixed_rows = jnp.where(live_rows[:, :, None, None], mixed_rows, 0.0)
    output = mixed_rows.reshape(batch_size, row_count, head_count * HD).astype(jnp.bfloat16)
    upstream = jnp.where(
        live_rows[:, :, None, None], cotangent.reshape(batch_size, row_count, head_count, HD), 0.0
    )
    grad_prob = jnp.einsum(
        "erhd,ekhd->ehrk", upstream, value_rows, preferred_element_type=jnp.float32
    )
    row_delta = jnp.sum(probability * grad_prob, axis=-1, keepdims=True)
    grad_score = (probability * (grad_prob - row_delta)).astype(jnp.bfloat16)
    grad_query = (
        jnp.einsum(
            "ehrk,ekhd->erhd",
            grad_score[:, :, :prompt_len, :],
            key_rows,
            preferred_element_type=jnp.float32,
        )
        * score_scale
    )
    grad_key = (
        jnp.einsum(
            "ehrk,erhd->ekhd",
            grad_score[:, :, :, :prompt_len],
            queries,
            preferred_element_type=jnp.float32,
        )
        * score_scale
    )
    grad_value = jnp.einsum(
        "ehrk,erhd->ekhd",
        probs_low[:, :, :, :prompt_len],
        upstream,
        preferred_element_type=jnp.float32,
    )
    cosine_lead = cosine_table[:prompt_len]
    sine_lead = sine_table[:prompt_len]
    flat_rows = batch_size * prompt_len
    grad_query = (
        unrotate(grad_query, cosine_lead, sine_lead)
        .astype(jnp.bfloat16)
        .reshape(flat_rows, head_count * HD)
    )
    grad_key = (
        unrotate(grad_key, cosine_lead, sine_lead)
        .astype(jnp.bfloat16)
        .reshape(flat_rows, head_count * HD)
    )
    grad_value = grad_value.astype(jnp.bfloat16).reshape(flat_rows, head_count * HD)
    grad_normed = (
        transpose_product(grad_query, w_query)
        + transpose_product(grad_key, w_key)
        + transpose_product(grad_value, w_value)
    )
    grad_normed = grad_normed.reshape(batch_size, prompt_len, model_width) * gain
    prompt_rows = wide_rows[:, :prompt_len]
    prompt_inv = inv_rms[:, :prompt_len, None]
    grad_rows = prompt_inv * grad_normed - prompt_rows * prompt_inv**3 * jnp.mean(
        grad_normed * prompt_rows, axis=-1, keepdims=True
    )
    return (output, grad_rows)


def on_device(text, prompts, gain, w_query, w_key, w_value, cotangent, task_of, lengths, slot):
    dp_count = lax.axis_size("dp")
    my_index = lax.axis_index("dp")
    ex_dev = text.shape[0]
    task_dev = prompts.shape[0]
    prompt_len = prompts.shape[1]
    example_count = slot.shape[0]
    task_count = task_dev * dp_count
    places = jnp.arange(example_count, dtype=jnp.int32)
    matching = slot[None, :] == places[:, None]
    task_slot = jnp.sum(jnp.where(matching, task_of[None, :], 0), axis=1)
    length_slot = jnp.sum(jnp.where(matching, lengths[None, :], 0), axis=1)
    first_place = my_index * ex_dev
    my_lengths = lax.dynamic_slice_in_dim(length_slot, first_place, ex_dev)
    task_ids = jnp.arange(task_count, dtype=jnp.int32)
    spread_text, spread_prompts = (
        lax.all_to_all(text, "dp", split_axis=2, concat_axis=0, tiled=True),
        lax.all_to_all(prompts, "dp", split_axis=2, concat_axis=0, tiled=True),
    )
    taking = matching.astype(jnp.bfloat16)
    placed_text = jnp.einsum(
        "se,erc->src", taking, spread_text, preferred_element_type=jnp.bfloat16
    )
    choosing = (task_slot[:, None] == task_ids[None, :]).astype(jnp.bfloat16)
    placed_prompts = jnp.einsum(
        "st,tpc->spc", choosing, spread_prompts, preferred_element_type=jnp.bfloat16
    )
    placed = jnp.concatenate([placed_prompts, placed_text], axis=1)
    placed = placed.reshape(dp_count, ex_dev, placed.shape[1], placed.shape[2])
    local_rows = lax.all_to_all(placed, "dp", split_axis=0, concat_axis=3, tiled=True)[0]
    full_rows = lax.all_gather(local_rows, "tensor", axis=2, tiled=True)
    output, grad_part = attention_window(
        full_rows, gain, w_query, w_key, w_value, cotangent, my_lengths, prompt_len
    )
    grad_share = lax.psum_scatter(grad_part, "tensor", scatter_dimension=2, tiled=True)
    spread_grads = lax.all_to_all(grad_share, "dp", split_axis=2, concat_axis=0, tiled=True)
    collecting = (task_ids[:, None] == task_slot[None, :]).astype(jnp.float32)
    per_task = jnp.einsum("ts,spc->tpc", collecting, spread_grads, precision=lax.Precision.HIGHEST)
    prompt_grad = lax.all_to_all(per_task, "dp", split_axis=0, concat_axis=2, tiled=True)
    return (output, prompt_grad)


MESH = pl.DeviceIdType.MESH
PAD_POS = 1 << 20


def dispatch_kernel(source_ref, task_ref, inp_ref, out_ref, recv, send, sem1, sem2, semz):
    n, m = lax.axis_size("dp"), lax.axis_size("tensor")
    me, t = lax.axis_index("dp"), lax.axis_index("tensor")
    right, left = lax.rem(t + 1, m), lax.rem(t + m - 1, m)
    split = inp_ref.shape[1] * 2 // 3

    barrier = pltpu.get_barrier_semaphore()
    for k in range(1, n):
        pl.semaphore_signal(
            barrier, inc=1, device_id=(lax.rem(me + k, n), t), device_id_type=MESH
        )
    for z in (left, right):
        pl.semaphore_signal(barrier, inc=1, device_id=(me, z), device_id_type=MESH)
    pl.semaphore_wait(barrier, n + 1)

    first = []
    for k in range(1, n):
        peer = lax.rem(me + k, n)
        copy = pltpu.make_async_remote_copy(
            src_ref=inp_ref.at[peer],
            dst_ref=recv.at[me],
            send_sem=sem1.at[0, k],
            recv_sem=sem1.at[1, k],
            device_id=(peer, t),
            device_id_type=MESH,
        )
        copy.start()
        first.append(copy)
    recv[me] = inp_ref[me]
    for copy in first:
        copy.wait_recv()

    second = []
    for k in range(1, n):
        peer = lax.rem(me + k, n)
        send[k, :split] = recv[source_ref[peer], :split]
        send[k, split:] = recv[task_ref[peer], split:]
        copy = pltpu.make_async_remote_copy(
            src_ref=send.at[k],
            dst_ref=out_ref.at[t, me],
            send_sem=sem2.at[0, k],
            recv_sem=sem2.at[1, k],
            device_id=(peer, t),
            device_id_type=MESH,
        )
        copy.start()
        second.append(copy)
    out_ref[t, me, :split] = recv[source_ref[me], :split]
    out_ref[t, me, split:] = recv[task_ref[me], split:]

    def hop(origin, k, distance, way):
        chunk = lax.rem(me + n - k, n)
        place = out_ref.at[origin, chunk]
        copy = pltpu.make_async_remote_copy(
            src_ref=place,
            dst_ref=place,
            send_sem=semz.at[0, way, distance, k],
            recv_sem=semz.at[1, way, distance, k],
            device_id=(me, left if way else right),
            device_id_type=MESH,
        )
        copy.start()
        return copy

    def reach(k, way):
        half = m // 2
        long_way = k % 2
        return half if way == long_way else m - 1 - half

    hops = {}
    for k in range(n):
        if k:
            second[k - 1].wait_recv()
        for way in (0, 1):
            if reach(k, way) >= 1:
                hops[way, 1, k] = hop(t, k, 1, way)
    for distance in range(1, m // 2 + 1):
        for k in range(n):
            for way in (0, 1):
                if distance <= reach(k, way):
                    hops[way, distance, k].wait_recv()
                    if distance < reach(k, way):
                        origin = lax.rem(t + (m - distance if way == 0 else distance), m)
                        hops[way, distance + 1, k] = hop(origin, k, distance + 1, way)
    for copy in first + second:
        copy.wait_send()
    for copy in hops.values():
        copy.wait_send()


def collect_kernel(weight_ref, part_ref, out_ref, recvz, send1, recv1, send2, recv2, semz, sem1, sem2):
    n, m = lax.axis_size("dp"), lax.axis_size("tensor")
    me, t = lax.axis_index("dp"), lax.axis_index("tensor")
    f32 = jnp.float32

    barrier = pltpu.get_barrier_semaphore()
    for k in range(1, n):
        pl.semaphore_signal(
            barrier, inc=1, device_id=(lax.rem(me + k, n), t), device_id_type=MESH
        )
    for k in range(1, m):
        pl.semaphore_signal(
            barrier, inc=1, device_id=(me, lax.rem(t + k, m)), device_id_type=MESH
        )
    pl.semaphore_wait(barrier, n + m - 2)

    copies = []
    for k in range(1, m):
        peer = lax.rem(t + k, m)
        copy = pltpu.make_async_remote_copy(
            src_ref=part_ref.at[peer],
            dst_ref=recvz.at[k],
            send_sem=semz.at[0, k],
            recv_sem=semz.at[1, k],
            device_id=(me, peer),
            device_id_type=MESH,
        )
        copy.start()
        copies.append(copy)
    for copy in copies:
        copy.wait_recv()
    firsts = []
    for k in range(n):
        chunk = lax.rem(me + k, n)
        total = part_ref[t, chunk].astype(f32)
        for z in range(1, m):
            total = total + recvz[z, chunk].astype(f32)
        if k == 0:
            recv1[me] = total.astype(recv1.dtype)
            continue
        send1[k] = total.astype(send1.dtype)
        copy = pltpu.make_async_remote_copy(
            src_ref=send1.at[k],
            dst_ref=recv1.at[me],
            send_sem=sem1.at[0, k],
            recv_sem=sem1.at[1, k],
            device_id=(chunk, t),
            device_id_type=MESH,
        )
        copy.start()
        firsts.append(copy)
    for copy in firsts:
        copy.wait_recv()
    seconds = []
    for k in range(n):
        peer = lax.rem(me + k, n)
        total = weight_ref[peer, 0] * recv1[0].astype(f32)
        for s in range(1, n):
            total = total + weight_ref[peer, s] * recv1[s].astype(f32)
        if k == 0:
            recv2[me] = total.astype(recv2.dtype)
            continue
        send2[k] = total.astype(send2.dtype)
        copy = pltpu.make_async_remote_copy(
            src_ref=send2.at[k],
            dst_ref=recv2.at[me],
            send_sem=sem2.at[0, k],
            recv_sem=sem2.at[1, k],
            device_id=(peer, t),
            device_id_type=MESH,
        )
        copy.start()
        seconds.append(copy)
    for copy in seconds:
        copy.wait_recv()
    for chunk in range(n):
        out_ref[chunk] = recv2[chunk].astype(out_ref.dtype)
    for copy in copies + firsts + seconds:
        copy.wait_send()


def dot_nn(a, b):
    return jnp.dot(a, b, preferred_element_type=jnp.float32)


def dot_nt(a, b):
    return lax.dot_general(a, b, (((1,), (1,)), ((), ())), preferred_element_type=jnp.float32)


def dot_tn(a, b):
    return lax.dot_general(a, b, (((0,), (0,)), ((), ())), preferred_element_type=jnp.float32)


def compute_kernel(
    n, limit_ref, x_ref, gain_ref, cos_ref, sin_ref, posr_ref, posc_ref,
    wq_ref, wk_ref, wv_ref, cot_ref, out_ref, grad_ref, normed, acc, inv_ref,
):
    step = pl.program_id(0)
    m, rows, width = x_ref.shape
    model_width = m * width
    f32, bf16 = jnp.float32, jnp.bfloat16
    chunk = rows // n
    lead = chunk // 3
    limit = limit_ref[0]

    def prompt_rows(value):
        return value.reshape(n, chunk, value.shape[-1])[:, chunk - lead :].reshape(
            n * lead, value.shape[-1]
        )

    @pl.when(step == 0)
    def _():
        square = jnp.zeros((rows, 1), f32)
        for z in range(m):
            wide = x_ref[z].astype(f32)
            square = square + jnp.sum(wide * wide, axis=1, keepdims=True)
        inv = lax.rsqrt(square * (1.0 / model_width) + 1e-05)
        inv_ref[...] = jnp.broadcast_to(inv, inv_ref.shape)
        for z in range(m):
            normed[z] = (x_ref[z].astype(f32) * inv * gain_ref[z]).astype(bf16)

    def project(w_ref):
        total = dot_nn(normed[0], w_ref[:width])
        for z in range(1, m):
            total = total + dot_nn(normed[z], w_ref[z * width : (z + 1) * width])
        return total

    cosine, sine = cos_ref[...], sin_ref[...]
    cosine_p, sine_p = prompt_rows(cosine), prompt_rows(sine)
    row_pos, col_pos = posr_ref[...], posc_ref[...]
    allowed = (col_pos <= row_pos) & (col_pos < limit)
    live = row_pos < limit
    scale = 1.0 / math.sqrt(HD)
    q_all, k_all, v_all = project(wq_ref), project(wk_ref), project(wv_ref)
    grads_q, grads_k, grads_v = [], [], []
    for h in range(wq_ref.shape[1] // HD):
        at = slice(h * HD, (h + 1) * HD)
        q, k, v = q_all[:, at], k_all[:, at], v_all[:, at].astype(bf16)
        q = (q * cosine + pltpu.roll(q, HD // 2, 1) * sine).astype(bf16)
        k = (k * cosine + pltpu.roll(k, HD // 2, 1) * sine).astype(bf16)
        scores = jnp.where(allowed, dot_nt(q, k) * scale, -1e30)
        peak = jnp.max(scores, axis=1, keepdims=True)
        weights = jnp.where(allowed, jnp.exp(scores - peak), 0.0)
        probs = weights / jnp.sum(weights, axis=1, keepdims=True)
        low = probs.astype(bf16)
        out_ref[:, at] = jnp.where(live, dot_nn(low, v), 0.0).astype(bf16)
        upstream = jnp.where(live, cot_ref[:, at].astype(f32), 0.0).astype(bf16)
        grad_prob = dot_nt(upstream, v)
        delta = jnp.sum(probs * grad_prob, axis=1, keepdims=True)
        grad_score = probs * (grad_prob - delta)
        low_score = grad_score.astype(bf16)
        gq = dot_nn(prompt_rows(grad_score).astype(bf16), k) * scale
        gk = prompt_rows(dot_tn(low_score, q)) * scale
        gv = prompt_rows(dot_tn(low, upstream))
        gq = gq * cosine_p - pltpu.roll(gq, HD // 2, 1) * sine_p
        gk = gk * cosine_p - pltpu.roll(gk, HD // 2, 1) * sine_p
        grads_q.append(gq.astype(bf16))
        grads_k.append(gk.astype(bf16))
        grads_v.append(gv.astype(bf16))
    grads_q = jnp.concatenate(grads_q, axis=1)
    grads_k = jnp.concatenate(grads_k, axis=1)
    grads_v = jnp.concatenate(grads_v, axis=1)
    first = step == 0
    for z in range(m):
        at = slice(z * width, (z + 1) * width)
        total = (
            dot_nt(grads_q, wq_ref[at])
            + dot_nt(grads_k, wk_ref[at])
            + dot_nt(grads_v, wv_ref[at])
        )
        acc[z] = jnp.where(first, total, acc[z] + total)

    @pl.when(step == pl.num_programs(0) - 1)
    def _():
        inv = prompt_rows(inv_ref[...])[:, :1]
        dots = jnp.zeros((n * lead, 1), f32)
        for z in range(m):
            scaled = acc[z] * gain_ref[z]
            acc[z] = scaled
            wide = prompt_rows(x_ref[z].astype(f32))
            dots = dots + jnp.sum(scaled * wide, axis=1, keepdims=True)
        factor = inv * inv * inv * (dots * (1.0 / model_width))
        for z in range(m):
            wide = prompt_rows(x_ref[z].astype(f32))
            grad_ref[z] = (inv * acc[z] - wide * factor).astype(bf16)


def fast_device(text, prompts, gain, w_query, w_key, w_value, cotangent, task_of, lengths, slot):
    n, m = lax.axis_size("dp"), lax.axis_size("tensor")
    f32, bf16 = jnp.float32, jnp.bfloat16
    me = lax.axis_index("dp")
    seq, width = text.shape[1], text.shape[2]
    p_len = prompts.shape[1]
    ct = seq // n
    cp = ct // 2
    chunk = ct + cp
    rows = n * chunk
    heads = w_query.shape[1]
    places = jnp.arange(n, dtype=jnp.int32)
    matching = slot[None, :] == places[:, None]
    source_slot = jnp.sum(jnp.where(matching, places[None, :], 0), axis=1)
    task_slot = jnp.sum(jnp.where(matching, task_of[None, :], 0), axis=1)
    length_slot = jnp.sum(jnp.where(matching, lengths[None, :], 0), axis=1)
    limit = p_len + lax.dynamic_slice_in_dim(length_slot, me, 1)
    weight = (places[:, None] == task_slot[None, :]).astype(f32)

    def interleave(tail, lead):
        lead = jnp.pad(lead, ((0, n * cp - p_len), (0, 0)))
        parts = [tail.reshape(n, ct, -1), lead.reshape(n, cp, -1)]
        return jnp.concatenate(parts, axis=1)

    smem = pl.BlockSpec(memory_space=pltpu.SMEM)
    vmem = pl.BlockSpec(memory_space=pltpu.VMEM)
    chunks = interleave(text[0], prompts[0])
    gathered = pl.pallas_call(
        dispatch_kernel,
        out_shape=jax.ShapeDtypeStruct((m, n, chunk, width), bf16),
        in_specs=[smem, smem, vmem],
        out_specs=vmem,
        scratch_shapes=[
            pltpu.VMEM((n, chunk, width), bf16),
            pltpu.VMEM((n, chunk, width), bf16),
            pltpu.SemaphoreType.DMA((2, n)),
            pltpu.SemaphoreType.DMA((2, n)),
            pltpu.SemaphoreType.DMA((2, 2, m // 2 + 1, n)),
        ],
        compiler_params=pltpu.CompilerParams(collective_id=0, has_side_effects=True),
    )(source_slot, task_slot, chunks)
    x = gathered.reshape(m, rows, width)

    row = jnp.arange(rows, dtype=jnp.int32)
    j, i = row // chunk, row % chunk
    lead_pos = j * cp + i - ct
    lead_pos = jnp.where(lead_pos < p_len, lead_pos, PAD_POS)
    pos = jnp.where(i < ct, p_len + j * ct + i, lead_pos)
    half = HD // 2
    frequency = 10000.0 ** (-jnp.arange(half, dtype=f32) / half)
    angle = jnp.where(pos < PAD_POS, pos, 0).astype(f32)[:, None] * frequency[None, :]
    cosine = jnp.concatenate([jnp.cos(angle)] * 2, axis=1)
    sine = jnp.concatenate([-jnp.sin(angle), jnp.sin(angle)], axis=1)
    cot = interleave(cotangent[0, p_len:], cotangent[0, :p_len]).reshape(rows, heads)
    group = 2 * HD if heads % (2 * HD) == 0 else HD

    def whole(*shape):
        return pl.BlockSpec(shape, lambda g: (0,) * len(shape))

    w_spec = pl.BlockSpec((m * width, group), lambda g: (0, g))
    r_spec = pl.BlockSpec((rows, group), lambda g: (0, g))
    out, part = pl.pallas_call(
        functools.partial(compute_kernel, n),
        grid=(heads // group,),
        out_shape=(
            jax.ShapeDtypeStruct((rows, heads), bf16),
            jax.ShapeDtypeStruct((m, n * cp, width), bf16),
        ),
        in_specs=[
            smem,
            whole(m, rows, width),
            whole(m, 1, width),
            whole(rows, HD),
            whole(rows, HD),
            whole(rows, 1),
            whole(1, rows),
            w_spec,
            w_spec,
            w_spec,
            r_spec,
        ],
        out_specs=(r_spec, whole(m, n * cp, width)),
        scratch_shapes=[
            pltpu.VMEM((m, rows, width), bf16),
            pltpu.VMEM((m, n * cp, width), f32),
            pltpu.VMEM((rows, HD), f32),
        ],
        compiler_params=pltpu.CompilerParams(vmem_limit_bytes=60 * 2**20),
    )(
        limit, x, gain.reshape(m, 1, width), cosine, sine, pos[:, None], pos[None, :],
        w_query, w_key, w_value, cot,
    )
    collected = pl.pallas_call(
        collect_kernel,
        out_shape=jax.ShapeDtypeStruct((n, cp, width), f32),
        in_specs=[smem, vmem],
        out_specs=vmem,
        scratch_shapes=[
            pltpu.VMEM((m, n, cp, width), bf16),
            pltpu.VMEM((n, cp, width), bf16),
            pltpu.VMEM((n, cp, width), bf16),
            pltpu.VMEM((n, cp, width), bf16),
            pltpu.VMEM((n, cp, width), bf16),
            pltpu.SemaphoreType.DMA((2, m)),
            pltpu.SemaphoreType.DMA((2, n)),
            pltpu.SemaphoreType.DMA((2, n)),
        ],
        compiler_params=pltpu.CompilerParams(collective_id=1, has_side_effects=True),
    )(weight, part.reshape(m, n, cp, width))
    prompt_grad = collected.reshape(n * cp, width)[:p_len][None]
    out = out.reshape(n, chunk, heads)
    lead = out[:, ct:].reshape(n * cp, heads)[:p_len]
    attn_out = jnp.concatenate([lead, out[:, :ct].reshape(seq, heads)], axis=0)[None]
    return (attn_out, prompt_grad)


def choose(text, prompts, *rest):
    n, m = lax.axis_size("dp"), lax.axis_size("tensor")
    seq, p_len = text.shape[1], prompts.shape[1]
    fits = (
        text.shape[0] == 1
        and prompts.shape[0] == 1
        and m >= 3
        and n >= 2
        and seq % (32 * n) == 0
        and p_len <= seq // 2
        and text.shape[2] % 128 == 0
    )
    return (fast_device if fits else on_device)(text, prompts, *rest)


def solution(mesh):
    in_specs = (
        P("dp", None, "tensor"),
        P("dp", None, "tensor"),
        P(),
        P(None, "tensor"),
        P(None, "tensor"),
        P(None, "tensor"),
        P("dp", None, "tensor"),
        P(),
        P(),
        P(),
    )
    out_specs = (P("dp", None, "tensor"), P("dp", None, "tensor"))
    return jax.shard_map(
        choose, mesh=mesh, in_specs=in_specs, out_specs=out_specs, check_vma=False
    )
```

```python
import functools
import math

import jax
import jax.numpy as jnp
from jax import lax
from jax.experimental import pallas as pl
from jax.experimental.pallas import tpu as pltpu
from jax.sharding import PartitionSpec as P

HD = 128


def rope_tables(row_count):
    half_dim = HD // 2
    frequency = 10000.0 ** (-jnp.arange(half_dim, dtype=jnp.float32) / half_dim)
    angle_table = jnp.arange(row_count, dtype=jnp.float32)[:, None] * frequency[None, :]
    return (jnp.cos(angle_table), jnp.sin(angle_table))


def rotate(vectors, cosine_table, sine_table):
    half_dim = vectors.shape[-1] // 2
    first_half = vectors[..., :half_dim]
    second_half = vectors[..., half_dim:]
    cosine_b = cosine_table[:, None, :]
    sine_b = sine_table[:, None, :]
    return jnp.concatenate(
        [
            first_half * cosine_b - second_half * sine_b,
            second_half * cosine_b + first_half * sine_b,
        ],
        axis=-1,
    )


def unrotate(vectors, cosine_table, sine_table):
    half_dim = vectors.shape[-1] // 2
    first_half = vectors[..., :half_dim]
    second_half = vectors[..., half_dim:]
    cosine_b = cosine_table[:, None, :]
    sine_b = sine_table[:, None, :]
    return jnp.concatenate(
        [
            first_half * cosine_b + second_half * sine_b,
            second_half * cosine_b - first_half * sine_b,
        ],
        axis=-1,
    )


def transpose_product(grad_low, matrix):
    return lax.dot_general(
        grad_low, matrix, (((1,), (1,)), ((), ())), preferred_element_type=jnp.float32
    )


def attention_window(full_rows, gain, w_query, w_key, w_value, cotangent, valid_rows, prompt_len):
    batch_size, row_count, model_width = full_rows.shape
    head_count = w_query.shape[1] // HD
    wide_rows = full_rows.astype(jnp.float32)
    inv_rms = lax.rsqrt(jnp.mean(wide_rows * wide_rows, axis=-1) + 1e-05)
    normed = (
        (wide_rows * inv_rms[..., None] * gain)
        .astype(jnp.bfloat16)
        .reshape(batch_size * row_count, model_width)
    )
    cosine_table, sine_table = rope_tables(row_count)

    def project(matrix):
        return jnp.dot(normed, matrix, preferred_element_type=jnp.float32).reshape(
            batch_size, row_count, head_count, HD
        )

    queries = rotate(project(w_query), cosine_table, sine_table).astype(jnp.bfloat16)
    key_rows = rotate(project(w_key), cosine_table, sine_table).astype(jnp.bfloat16)
    value_rows = project(w_value).astype(jnp.bfloat16)
    score_scale = 1.0 / math.sqrt(HD)
    scores = (
        jnp.einsum("erhd,ekhd->ehrk", queries, key_rows, preferred_element_type=jnp.float32)
        * score_scale
    )
    rows_at = jnp.arange(row_count, dtype=jnp.int32)
    row_limit = prompt_len + valid_rows
    allowed = (rows_at[None, None, :] <= rows_at[None, :, None]) & (
        rows_at[None, None, :] < row_limit[:, None, None]
    )
    allowed = allowed[:, None]
    scores = jnp.where(allowed, scores, -1e30)
    row_peak = jnp.max(scores, axis=-1, keepdims=True)
    weights = jnp.where(allowed, jnp.exp(scores - row_peak), 0.0)
    probability = weights / jnp.sum(weights, axis=-1, keepdims=True)
    probs_low = probability.astype(jnp.bfloat16)
    live_rows = rows_at[None, :] < row_limit[:, None]
    mixed_rows = jnp.einsum(
        "ehrk,ekhd->erhd", probs_low, value_rows, preferred_element_type=jnp.float32
    )
    mixed_rows = jnp.where(live_rows[:, :, None, None], mixed_rows, 0.0)
    output = mixed_rows.reshape(batch_size, row_count, head_count * HD).astype(jnp.bfloat16)
    upstream = jnp.where(
        live_rows[:, :, None, None], cotangent.reshape(batch_size, row_count, head_count, HD), 0.0
    )
    grad_prob = jnp.einsum(
        "erhd,ekhd->ehrk", upstream, value_rows, preferred_element_type=jnp.float32
    )
    row_delta = jnp.sum(probability * grad_prob, axis=-1, keepdims=True)
    grad_score = (probability * (grad_prob - row_delta)).astype(jnp.bfloat16)
    grad_query = (
        jnp.einsum(
            "ehrk,ekhd->erhd",
            grad_score[:, :, :prompt_len, :],
            key_rows,
            preferred_element_type=jnp.float32,
        )
        * score_scale
    )
    grad_key = (
        jnp.einsum(
            "ehrk,erhd->ekhd",
            grad_score[:, :, :, :prompt_len],
            queries,
            preferred_element_type=jnp.float32,
        )
        * score_scale
    )
    grad_value = jnp.einsum(
        "ehrk,erhd->ekhd",
        probs_low[:, :, :, :prompt_len],
        upstream,
        preferred_element_type=jnp.float32,
    )
    cosine_lead = cosine_table[:prompt_len]
    sine_lead = sine_table[:prompt_len]
    flat_rows = batch_size * prompt_len
    grad_query = (
        unrotate(grad_query, cosine_lead, sine_lead)
        .astype(jnp.bfloat16)
        .reshape(flat_rows, head_count * HD)
    )
    grad_key = (
        unrotate(grad_key, cosine_lead, sine_lead)
        .astype(jnp.bfloat16)
        .reshape(flat_rows, head_count * HD)
    )
    grad_value = grad_value.astype(jnp.bfloat16).reshape(flat_rows, head_count * HD)
    grad_normed = (
        transpose_product(grad_query, w_query)
        + transpose_product(grad_key, w_key)
        + transpose_product(grad_value, w_value)
    )
    grad_normed = grad_normed.reshape(batch_size, prompt_len, model_width) * gain
    prompt_rows = wide_rows[:, :prompt_len]
    prompt_inv = inv_rms[:, :prompt_len, None]
    grad_rows = prompt_inv * grad_normed - prompt_rows * prompt_inv**3 * jnp.mean(
        grad_normed * prompt_rows, axis=-1, keepdims=True
    )
    return (output, grad_rows)


def on_device(text, prompts, gain, w_query, w_key, w_value, cotangent, task_of, lengths, slot):
    dp_count = lax.axis_size("dp")
    my_index = lax.axis_index("dp")
    ex_dev = text.shape[0]
    task_dev = prompts.shape[0]
    prompt_len = prompts.shape[1]
    example_count = slot.shape[0]
    task_count = task_dev * dp_count
    places = jnp.arange(example_count, dtype=jnp.int32)
    matching = slot[None, :] == places[:, None]
    task_slot = jnp.sum(jnp.where(matching, task_of[None, :], 0), axis=1)
    length_slot = jnp.sum(jnp.where(matching, lengths[None, :], 0), axis=1)
    first_place = my_index * ex_dev
    my_lengths = lax.dynamic_slice_in_dim(length_slot, first_place, ex_dev)
    task_ids = jnp.arange(task_count, dtype=jnp.int32)
    spread_text, spread_prompts = (
        lax.all_to_all(text, "dp", split_axis=2, concat_axis=0, tiled=True),
        lax.all_to_all(prompts, "dp", split_axis=2, concat_axis=0, tiled=True),
    )
    taking = matching.astype(jnp.bfloat16)
    placed_text = jnp.einsum(
        "se,erc->src", taking, spread_text, preferred_element_type=jnp.bfloat16
    )
    choosing = (task_slot[:, None] == task_ids[None, :]).astype(jnp.bfloat16)
    placed_prompts = jnp.einsum(
        "st,tpc->spc", choosing, spread_prompts, preferred_element_type=jnp.bfloat16
    )
    placed = jnp.concatenate([placed_prompts, placed_text], axis=1)
    placed = placed.reshape(dp_count, ex_dev, placed.shape[1], placed.shape[2])
    local_rows = lax.all_to_all(placed, "dp", split_axis=0, concat_axis=3, tiled=True)[0]
    full_rows = lax.all_gather(local_rows, "tensor", axis=2, tiled=True)
    output, grad_part = attention_window(
        full_rows, gain, w_query, w_key, w_value, cotangent, my_lengths, prompt_len
    )
    grad_share = lax.psum_scatter(grad_part, "tensor", scatter_dimension=2, tiled=True)
    spread_grads = lax.all_to_all(grad_share, "dp", split_axis=2, concat_axis=0, tiled=True)
    collecting = (task_ids[:, None] == task_slot[None, :]).astype(jnp.float32)
    per_task = jnp.einsum("ts,spc->tpc", collecting, spread_grads, precision=lax.Precision.HIGHEST)
    prompt_grad = lax.all_to_all(per_task, "dp", split_axis=0, concat_axis=2, tiled=True)
    return (output, prompt_grad)


MESH = pl.DeviceIdType.MESH
PAD_POS = 1 << 20


def dot_nn(a, b):
    return jnp.dot(a, b, preferred_element_type=jnp.float32)


def dot_nt(a, b):
    return lax.dot_general(a, b, (((1,), (1,)), ((), ())), preferred_element_type=jnp.float32)


def dot_tn(a, b):
    return lax.dot_general(a, b, (((0,), (0,)), ((), ())), preferred_element_type=jnp.float32)


def step_kernel(
    p_len, slot_ref, task_ref, length_ref, inp_ref, gain_ref, cos_ref, sin_ref, posr_ref, posc_ref,
    cot_ref, wq_hbm, wk_hbm, wv_hbm, out_ref, grad_ref,
    w_ref, recv, send, full, squares, qkv, grads, inv_ref, acc, part, recvz, send1, recv1, send2, recv2,
    semw, sem1, sem2, semz, semq, semg, sem3, sem4,
):
    n, m = lax.axis_size("dp"), lax.axis_size("tensor")
    me, t = lax.axis_index("dp"), lax.axis_index("tensor")
    f32, bf16 = jnp.float32, jnp.bfloat16
    right, left = lax.rem(t + 1, m), lax.rem(t + m - 1, m)
    _, chunk, width = inp_ref.shape
    blocks, model_width, group = w_ref.shape
    per = blocks // 3
    rows = n * chunk
    lead = chunk // 3
    split = chunk - lead

    def pick(place, values):
        total = jnp.int32(0)
        for e in range(n):
            total = jnp.maximum(total, jnp.where(slot_ref[e] == place, values(e), 0))
        return total

    def source_of(place):
        return pick(place, lambda e: e)

    def task_at(place):
        return pick(place, lambda e: task_ref[e])

    def remote(src, dst, sems, device):
        copy = pltpu.make_async_remote_copy(
            src_ref=src,
            dst_ref=dst,
            send_sem=sems[0],
            recv_sem=sems[1],
            device_id=device,
            device_id_type=MESH,
        )
        copy.start()
        return copy

    loads = []
    for i, hbm in enumerate((wq_hbm, wk_hbm, wv_hbm)):
        for g in range(per):
            at = i * per + g
            load = pltpu.make_async_copy(
                hbm.at[:, g * group : (g + 1) * group], w_ref.at[at], semw.at[at]
            )
            load.start()
            loads.append(load)

    barrier = pltpu.get_barrier_semaphore()
    for k in range(1, n):
        pl.semaphore_signal(
            barrier, inc=1, device_id=(lax.rem(me + k, n), t), device_id_type=MESH
        )
    for k in range(1, m):
        pl.semaphore_signal(
            barrier, inc=1, device_id=(me, lax.rem(t + k, m)), device_id_type=MESH
        )
    pl.semaphore_wait(barrier, n + m - 2)

    first = []
    for k in range(1, n):
        peer = lax.rem(me + k, n)
        sems = (sem1.at[0, k], sem1.at[1, k])
        first.append(remote(inp_ref.at[peer], recv.at[me], sems, (peer, t)))
    recv[me] = inp_ref[me]
    for copy in first:
        copy.wait_recv()

    second = []
    for k in range(1, n):
        peer = lax.rem(me + k, n)
        send[k, :split] = recv[source_of(peer), :split]
        send[k, split:] = recv[task_at(peer), split:]
        sems = (sem2.at[0, k], sem2.at[1, k])
        second.append(remote(send.at[k], full.at[t, me], sems, (peer, t)))
    full[t, me, :split] = recv[source_of(me), :split]
    full[t, me, split:] = recv[task_at(me), split:]

    def hop(origin, k, distance, way):
        place = full.at[origin, lax.rem(me + n - k, n)]
        sems = (semz.at[0, way, distance, k], semz.at[1, way, distance, k])
        return remote(place, place, sems, (me, left if way else right))

    def reach(k, way):
        half = m // 2
        return half if way == k % 2 else m - 1 - half

    hops = {}
    for k in range(n):
        if k:
            second[k - 1].wait_recv()
        for way in (0, 1):
            hops[way, 1, k] = hop(t, k, 1, way)

    own = full[t].reshape(rows, width).astype(f32)
    square = jnp.sum(own * own, axis=1, keepdims=True)
    squares[0] = jnp.broadcast_to(square, (rows, 128)).T[:8]
    shared = []
    for k in range(1, m):
        peer = lax.rem(t + k, m)
        sems = (semq.at[0, k], semq.at[1, k])
        shared.append(remote(squares.at[0], squares.at[k], sems, (me, peer)))

    def origin_of(distance, way):
        return lax.rem(t + (m - distance if way == 0 else distance), m)

    def receive(distance):
        for k in range(n):
            for way in (0, 1):
                if distance <= reach(k, way):
                    hops[way, distance, k].wait_recv()
                    if distance < reach(k, way):
                        origin = origin_of(distance, way)
                        hops[way, distance + 1, k] = hop(origin, k, distance + 1, way)

    def project(origin, fresh):
        wide = full[origin].reshape(rows, width).astype(f32)
        normed = (wide * inv_ref[:, :1] * gain_ref[origin]).astype(bf16)
        deep = pl.ds(pl.multiple_of(origin * width, width), width)

        def body(b, carry):
            product = dot_nn(normed, w_ref[b, deep, :])
            qkv[b] = product if fresh else qkv[b] + product
            return carry

        lax.fori_loop(0, blocks, body, 0)

    receive(1)
    for copy in shared:
        copy.wait_recv()
    square = squares[0]
    for k in range(1, m):
        square = square + squares[k]
    square = jnp.broadcast_to(square[:1], (128, rows)).T
    inv_ref[...] = lax.rsqrt(square * (1.0 / model_width) + 1e-05)
    for load in loads:
        load.wait()
    project(t, True)
    project(origin_of(1, 0), False)
    project(origin_of(1, 1), False)
    for distance in range(2, m // 2 + 1):
        receive(distance)
        project(origin_of(distance, 0), False)
        if 2 * distance != m:
            project(origin_of(distance, 1), False)

    def prompt_rows(value):
        return value.reshape(n, chunk, value.shape[-1])[:, split:].reshape(
            n * lead, value.shape[-1]
        )

    limit = p_len + pick(me, lambda e: length_ref[e])
    scale = 1.0 / math.sqrt(HD)

    def heads(g, carry):
        cosine, sine = cos_ref[...], sin_ref[...]
        cosine_p, sine_p = prompt_rows(cosine), prompt_rows(sine)
        row_pos, col_pos = posr_ref[...], posc_ref[...]
        allowed = (col_pos <= row_pos) & (col_pos < limit)
        live = row_pos < limit
        for h in range(group // HD):
            at = slice(h * HD, (h + 1) * HD)
            far = pl.ds(pl.multiple_of(g * group + h * HD, HD), HD)
            q, k = qkv[g, :, at], qkv[per + g, :, at]
            v = qkv[2 * per + g, :, at].astype(bf16)
            q = (q * cosine + pltpu.roll(q, HD // 2, 1) * sine).astype(bf16)
            k = (k * cosine + pltpu.roll(k, HD // 2, 1) * sine).astype(bf16)
            scores = jnp.where(allowed, dot_nt(q, k) * scale, -1e30)
            peak = jnp.max(scores, axis=1, keepdims=True)
            weights = jnp.where(allowed, jnp.exp(scores - peak), 0.0)
            probs = weights / jnp.sum(weights, axis=1, keepdims=True)
            low = probs.astype(bf16)
            out_ref[:, far] = jnp.where(live, dot_nn(low, v), 0.0).astype(bf16)
            upstream = jnp.where(live, cot_ref[:, far].astype(f32), 0.0).astype(bf16)
            grad_prob = dot_nt(upstream, v)
            delta = jnp.sum(probs * grad_prob, axis=1, keepdims=True)
            grad_score = probs * (grad_prob - delta)
            gq = dot_nn(prompt_rows(grad_score).astype(bf16), k) * scale
            gk = prompt_rows(dot_tn(grad_score.astype(bf16), q)) * scale
            gv = prompt_rows(dot_tn(low, upstream))
            gq = gq * cosine_p - pltpu.roll(gq, HD // 2, 1) * sine_p
            gk = gk * cosine_p - pltpu.roll(gk, HD // 2, 1) * sine_p
            grads[g, :, at] = gq.astype(bf16)
            grads[per + g, :, at] = gk.astype(bf16)
            grads[2 * per + g, :, at] = gv.astype(bf16)
        return carry

    lax.fori_loop(0, per, heads, 0)

    def prompts_of(z):
        return full[z, :, split:, :].astype(f32).reshape(n * lead, width)

    def back(z, dots):
        deep = pl.ds(pl.multiple_of(z * width, width), width)
        total = dot_nt(grads[0], w_ref[0, deep, :])
        for b in range(1, blocks):
            total = total + dot_nt(grads[b], w_ref[b, deep, :])
        total = total * gain_ref[z]
        acc[z] = total
        return dots + jnp.sum(total * prompts_of(z), axis=1, keepdims=True)

    dots = lax.fori_loop(0, m, back, jnp.zeros((n * lead, 1), f32))
    inv = prompt_rows(inv_ref[...])[:, :1]
    factor = inv * inv * inv * (dots * (1.0 / model_width))

    partial = {}
    for step in range(m):
        z = lax.rem(t + (2, 1, 3, 0)[step] if m == 4 else t + m - 1 - step, m)
        value = (inv * acc[z] - prompts_of(z) * factor).astype(bf16)
        part[z] = value.reshape(n, lead, width)
        if step < m - 1:
            for k in range(n):
                at = lax.rem(me + k, n)
                sems = (semg.at[0, step, k], semg.at[1, step, k])
                partial[step, k] = remote(part.at[z, at], recvz.at[step, at], sems, (me, z))

    third = []
    for k in range(n):
        at = lax.rem(me + k, n)
        total = part[t, at].astype(f32)
        for step in range(m - 1):
            partial[step, k].wait_recv()
            total = total + recvz[step, at].astype(f32)
        if k == 0:
            recv1[me] = total.astype(bf16)
            continue
        send1[k] = total.astype(bf16)
        sems = (sem3.at[0, k], sem3.at[1, k])
        third.append(remote(send1.at[k], recv1.at[me], sems, (at, t)))
    for copy in third:
        copy.wait_recv()
    tasks = [task_at(s) for s in range(n)]
    fourth = []
    for k in range(n):
        peer = lax.rem(me + k, n)
        total = jnp.zeros((lead, width), f32)
        for s in range(n):
            hit = jnp.where(tasks[s] == peer, 1.0, 0.0)
            total = total + hit * recv1[s].astype(f32)
        if k == 0:
            recv2[me] = total.astype(bf16)
            continue
        send2[k] = total.astype(bf16)
        sems = (sem4.at[0, k], sem4.at[1, k])
        fourth.append(remote(send2.at[k], recv2.at[me], sems, (peer, t)))
    for copy in fourth:
        copy.wait_recv()
    for at in range(n):
        grad_ref[at] = recv2[at].astype(f32)
    for copy in first + second + list(hops.values()) + shared:
        copy.wait_send()
    for copy in list(partial.values()) + third + fourth:
        copy.wait_send()


def fast_device(text, prompts, gain, w_query, w_key, w_value, cotangent, task_of, lengths, slot):
    n, m = lax.axis_size("dp"), lax.axis_size("tensor")
    f32, bf16 = jnp.float32, jnp.bfloat16
    seq, width = text.shape[1], text.shape[2]
    p_len = prompts.shape[1]
    ct = seq // n
    cp = ct // 2
    chunk = ct + cp
    rows = n * chunk
    heads = w_query.shape[1]

    def interleave(tail, lead):
        lead = jnp.pad(lead, ((0, n * cp - p_len), (0, 0)))
        parts = [tail.reshape(n, ct, -1), lead.reshape(n, cp, -1)]
        return jnp.concatenate(parts, axis=1)

    row = jnp.arange(rows, dtype=jnp.int32)
    j, i = row // chunk, row % chunk
    lead_pos = j * cp + i - ct
    lead_pos = jnp.where(lead_pos < p_len, lead_pos, PAD_POS)
    pos = jnp.where(i < ct, p_len + j * ct + i, lead_pos)
    half = HD // 2
    frequency = 10000.0 ** (-jnp.arange(half, dtype=f32) / half)
    angle = jnp.where(pos < PAD_POS, pos, 0).astype(f32)[:, None] * frequency[None, :]
    cosine = jnp.concatenate([jnp.cos(angle)] * 2, axis=1)
    sine = jnp.concatenate([-jnp.sin(angle), jnp.sin(angle)], axis=1)
    cot = interleave(cotangent[0, p_len:], cotangent[0, :p_len]).reshape(rows, heads)
    group = 2 * HD if heads % (2 * HD) == 0 else HD
    blocks = 3 * (heads // group)
    smem = pl.BlockSpec(memory_space=pltpu.SMEM)
    vmem = pl.BlockSpec(memory_space=pltpu.VMEM)
    hbm = pl.BlockSpec(memory_space=pl.ANY)
    dma = pltpu.SemaphoreType.DMA
    out, collected = pl.pallas_call(
        functools.partial(step_kernel, p_len),
        out_shape=(
            jax.ShapeDtypeStruct((rows, heads), bf16),
            jax.ShapeDtypeStruct((n, cp, width), f32),
        ),
        in_specs=[smem] * 3 + [vmem] * 7 + [hbm] * 3,
        out_specs=(vmem, vmem),
        scratch_shapes=[
            pltpu.VMEM((blocks, m * width, group), bf16),
            pltpu.VMEM((n, chunk, width), bf16),
            pltpu.VMEM((n, chunk, width), bf16),
            pltpu.VMEM((m, n, chunk, width), bf16),
            pltpu.VMEM((m, 8, rows), f32),
            pltpu.VMEM((blocks, rows, group), f32),
            pltpu.VMEM((blocks, n * cp, group), bf16),
            pltpu.VMEM((rows, 128), f32),
            pltpu.VMEM((m, n * cp, width), f32),
            pltpu.VMEM((m, n, cp, width), bf16),
            pltpu.VMEM((m - 1, n, cp, width), bf16),
            pltpu.VMEM((n, cp, width), bf16),
            pltpu.VMEM((n, cp, width), bf16),
            pltpu.VMEM((n, cp, width), bf16),
            pltpu.VMEM((n, cp, width), bf16),
            dma((blocks,)),
            dma((2, n)),
            dma((2, n)),
            dma((2, 2, m // 2 + 1, n)),
            dma((2, m)),
            dma((2, m, n)),
            dma((2, n)),
            dma((2, n)),
        ],
        compiler_params=pltpu.CompilerParams(
            collective_id=0, has_side_effects=True, vmem_limit_bytes=63 * 2**20
        ),
    )(
        slot, task_of, lengths, interleave(text[0], prompts[0]), gain.reshape(m, 1, width),
        cosine, sine, pos[:, None], pos[None, :], cot, w_query, w_key, w_value,
    )
    prompt_grad = collected.reshape(n * cp, width)[:p_len][None]
    out = out.reshape(n, chunk, heads)
    lead = out[:, ct:].reshape(n * cp, heads)[:p_len]
    attn_out = jnp.concatenate([lead, out[:, :ct].reshape(seq, heads)], axis=0)[None]
    return (attn_out, prompt_grad)


def choose(text, prompts, *rest):
    n, m = lax.axis_size("dp"), lax.axis_size("tensor")
    seq, p_len = text.shape[1], prompts.shape[1]
    fits = (
        text.shape[0] == 1
        and prompts.shape[0] == 1
        and m >= 3
        and n >= 2
        and seq % (32 * n) == 0
        and p_len <= seq // 2
        and text.shape[2] % 128 == 0
    )
    return (fast_device if fits else on_device)(text, prompts, *rest)


def solution(mesh):
    in_specs = (
        P("dp", None, "tensor"),
        P("dp", None, "tensor"),
        P(),
        P(None, "tensor"),
        P(None, "tensor"),
        P(None, "tensor"),
        P("dp", None, "tensor"),
        P(),
        P(),
        P(),
    )
    out_specs = (P("dp", None, "tensor"), P("dp", None, "tensor"))
    return jax.shard_map(
        choose, mesh=mesh, in_specs=in_specs, out_specs=out_specs, check_vma=False
    )
```

```python
import functools
import math

import jax
import jax.numpy as jnp
import numpy as np
from jax import lax
from jax.experimental import pallas as pl
from jax.experimental.pallas import tpu as pltpu
from jax.sharding import PartitionSpec as P

HD = 128


def rope_tables(row_count):
    half_dim = HD // 2
    frequency = 10000.0 ** (-jnp.arange(half_dim, dtype=jnp.float32) / half_dim)
    angle_table = jnp.arange(row_count, dtype=jnp.float32)[:, None] * frequency[None, :]
    return (jnp.cos(angle_table), jnp.sin(angle_table))


def rotate(vectors, cosine_table, sine_table):
    half_dim = vectors.shape[-1] // 2
    first_half = vectors[..., :half_dim]
    second_half = vectors[..., half_dim:]
    cosine_b = cosine_table[:, None, :]
    sine_b = sine_table[:, None, :]
    return jnp.concatenate(
        [
            first_half * cosine_b - second_half * sine_b,
            second_half * cosine_b + first_half * sine_b,
        ],
        axis=-1,
    )


def unrotate(vectors, cosine_table, sine_table):
    half_dim = vectors.shape[-1] // 2
    first_half = vectors[..., :half_dim]
    second_half = vectors[..., half_dim:]
    cosine_b = cosine_table[:, None, :]
    sine_b = sine_table[:, None, :]
    return jnp.concatenate(
        [
            first_half * cosine_b + second_half * sine_b,
            second_half * cosine_b - first_half * sine_b,
        ],
        axis=-1,
    )


def transpose_product(grad_low, matrix):
    return lax.dot_general(
        grad_low, matrix, (((1,), (1,)), ((), ())), preferred_element_type=jnp.float32
    )


def attention_window(full_rows, gain, w_query, w_key, w_value, cotangent, valid_rows, prompt_len):
    batch_size, row_count, model_width = full_rows.shape
    head_count = w_query.shape[1] // HD
    wide_rows = full_rows.astype(jnp.float32)
    inv_rms = lax.rsqrt(jnp.mean(wide_rows * wide_rows, axis=-1) + 1e-05)
    normed = (
        (wide_rows * inv_rms[..., None] * gain)
        .astype(jnp.bfloat16)
        .reshape(batch_size * row_count, model_width)
    )
    cosine_table, sine_table = rope_tables(row_count)

    def project(matrix):
        return jnp.dot(normed, matrix, preferred_element_type=jnp.float32).reshape(
            batch_size, row_count, head_count, HD
        )

    queries = rotate(project(w_query), cosine_table, sine_table).astype(jnp.bfloat16)
    key_rows = rotate(project(w_key), cosine_table, sine_table).astype(jnp.bfloat16)
    value_rows = project(w_value).astype(jnp.bfloat16)
    score_scale = 1.0 / math.sqrt(HD)
    scores = (
        jnp.einsum("erhd,ekhd->ehrk", queries, key_rows, preferred_element_type=jnp.float32)
        * score_scale
    )
    rows_at = jnp.arange(row_count, dtype=jnp.int32)
    row_limit = prompt_len + valid_rows
    allowed = (rows_at[None, None, :] <= rows_at[None, :, None]) & (
        rows_at[None, None, :] < row_limit[:, None, None]
    )
    allowed = allowed[:, None]
    scores = jnp.where(allowed, scores, -1e30)
    row_peak = jnp.max(scores, axis=-1, keepdims=True)
    weights = jnp.where(allowed, jnp.exp(scores - row_peak), 0.0)
    probability = weights / jnp.sum(weights, axis=-1, keepdims=True)
    probs_low = probability.astype(jnp.bfloat16)
    live_rows = rows_at[None, :] < row_limit[:, None]
    mixed_rows = jnp.einsum(
        "ehrk,ekhd->erhd", probs_low, value_rows, preferred_element_type=jnp.float32
    )
    mixed_rows = jnp.where(live_rows[:, :, None, None], mixed_rows, 0.0)
    output = mixed_rows.reshape(batch_size, row_count, head_count * HD).astype(jnp.bfloat16)
    upstream = jnp.where(
        live_rows[:, :, None, None], cotangent.reshape(batch_size, row_count, head_count, HD), 0.0
    )
    grad_prob = jnp.einsum(
        "erhd,ekhd->ehrk", upstream, value_rows, preferred_element_type=jnp.float32
    )
    row_delta = jnp.sum(probability * grad_prob, axis=-1, keepdims=True)
    grad_score = (probability * (grad_prob - row_delta)).astype(jnp.bfloat16)
    grad_query = (
        jnp.einsum(
            "ehrk,ekhd->erhd",
            grad_score[:, :, :prompt_len, :],
            key_rows,
            preferred_element_type=jnp.float32,
        )
        * score_scale
    )
    grad_key = (
        jnp.einsum(
            "ehrk,erhd->ekhd",
            grad_score[:, :, :, :prompt_len],
            queries,
            preferred_element_type=jnp.float32,
        )
        * score_scale
    )
    grad_value = jnp.einsum(
        "ehrk,erhd->ekhd",
        probs_low[:, :, :, :prompt_len],
        upstream,
        preferred_element_type=jnp.float32,
    )
    cosine_lead = cosine_table[:prompt_len]
    sine_lead = sine_table[:prompt_len]
    flat_rows = batch_size * prompt_len
    grad_query = (
        unrotate(grad_query, cosine_lead, sine_lead)
        .astype(jnp.bfloat16)
        .reshape(flat_rows, head_count * HD)
    )
    grad_key = (
        unrotate(grad_key, cosine_lead, sine_lead)
        .astype(jnp.bfloat16)
        .reshape(flat_rows, head_count * HD)
    )
    grad_value = grad_value.astype(jnp.bfloat16).reshape(flat_rows, head_count * HD)
    grad_normed = (
        transpose_product(grad_query, w_query)
        + transpose_product(grad_key, w_key)
        + transpose_product(grad_value, w_value)
    )
    grad_normed = grad_normed.reshape(batch_size, prompt_len, model_width) * gain
    prompt_rows = wide_rows[:, :prompt_len]
    prompt_inv = inv_rms[:, :prompt_len, None]
    grad_rows = prompt_inv * grad_normed - prompt_rows * prompt_inv**3 * jnp.mean(
        grad_normed * prompt_rows, axis=-1, keepdims=True
    )
    return (output, grad_rows)


def on_device(text, prompts, gain, w_query, w_key, w_value, cotangent, task_of, lengths, slot):
    dp_count = lax.axis_size("dp")
    my_index = lax.axis_index("dp")
    ex_dev = text.shape[0]
    task_dev = prompts.shape[0]
    prompt_len = prompts.shape[1]
    example_count = slot.shape[0]
    task_count = task_dev * dp_count
    places = jnp.arange(example_count, dtype=jnp.int32)
    matching = slot[None, :] == places[:, None]
    task_slot = jnp.sum(jnp.where(matching, task_of[None, :], 0), axis=1)
    length_slot = jnp.sum(jnp.where(matching, lengths[None, :], 0), axis=1)
    first_place = my_index * ex_dev
    my_lengths = lax.dynamic_slice_in_dim(length_slot, first_place, ex_dev)
    task_ids = jnp.arange(task_count, dtype=jnp.int32)
    spread_text, spread_prompts = (
        lax.all_to_all(text, "dp", split_axis=2, concat_axis=0, tiled=True),
        lax.all_to_all(prompts, "dp", split_axis=2, concat_axis=0, tiled=True),
    )
    taking = matching.astype(jnp.bfloat16)
    placed_text = jnp.einsum(
        "se,erc->src", taking, spread_text, preferred_element_type=jnp.bfloat16
    )
    choosing = (task_slot[:, None] == task_ids[None, :]).astype(jnp.bfloat16)
    placed_prompts = jnp.einsum(
        "st,tpc->spc", choosing, spread_prompts, preferred_element_type=jnp.bfloat16
    )
    placed = jnp.concatenate([placed_prompts, placed_text], axis=1)
    placed = placed.reshape(dp_count, ex_dev, placed.shape[1], placed.shape[2])
    local_rows = lax.all_to_all(placed, "dp", split_axis=0, concat_axis=3, tiled=True)[0]
    full_rows = lax.all_gather(local_rows, "tensor", axis=2, tiled=True)
    output, grad_part = attention_window(
        full_rows, gain, w_query, w_key, w_value, cotangent, my_lengths, prompt_len
    )
    grad_share = lax.psum_scatter(grad_part, "tensor", scatter_dimension=2, tiled=True)
    spread_grads = lax.all_to_all(grad_share, "dp", split_axis=2, concat_axis=0, tiled=True)
    collecting = (task_ids[:, None] == task_slot[None, :]).astype(jnp.float32)
    per_task = jnp.einsum("ts,spc->tpc", collecting, spread_grads, precision=lax.Precision.HIGHEST)
    prompt_grad = lax.all_to_all(per_task, "dp", split_axis=0, concat_axis=2, tiled=True)
    return (output, prompt_grad)


MESH = pl.DeviceIdType.MESH
PAD_POS = 1 << 20


def dot_nn(a, b):
    return jnp.dot(a, b, preferred_element_type=jnp.float32)


def dot_nt(a, b):
    return lax.dot_general(a, b, (((1,), (1,)), ((), ())), preferred_element_type=jnp.float32)


def dot_tn(a, b):
    return lax.dot_general(a, b, (((0,), (0,)), ((), ())), preferred_element_type=jnp.float32)


def step_kernel(
    p_len, slot_ref, task_ref, length_ref, inp_ref, gain_ref, cos_ref, sin_ref, posr_ref, posc_ref,
    cot_ref, wq_hbm, wk_hbm, wv_hbm, out_ref, grad_ref,
    w_ref, recv, send, full, squares, qkv, grads, inv_ref, acc, part, recvz, send1, recv1, send2, recv2,
    semw, sem1, sem2, semz, semq, semg, sem3, sem4,
):
    n, m = lax.axis_size("dp"), lax.axis_size("tensor")
    me, t = lax.axis_index("dp"), lax.axis_index("tensor")
    f32, bf16 = jnp.float32, jnp.bfloat16
    right, left = lax.rem(t + 1, m), lax.rem(t + m - 1, m)
    _, chunk, width = inp_ref.shape
    blocks, model_width, group = w_ref.shape
    per = blocks // 3
    rows = n * chunk
    lead = chunk // 3
    split = chunk - lead

    def pick(place, values):
        total = jnp.int32(0)
        for e in range(n):
            total = jnp.maximum(total, jnp.where(slot_ref[e] == place, values(e), 0))
        return total

    def source_of(place):
        return pick(place, lambda e: e)

    def task_at(place):
        return pick(place, lambda e: task_ref[e])

    def remote(src, dst, sems, device, needed=None):
        copy = pltpu.make_async_remote_copy(
            src_ref=src,
            dst_ref=dst,
            send_sem=sems[0],
            recv_sem=sems[1],
            device_id=device,
            device_id_type=MESH,
        )
        if needed is None:
            copy.start()
        else:
            pl.when(needed)(copy.start)
        return copy

    def holds(at):
        return at * lead < p_len

    loads = []
    for i, hbm in enumerate((wq_hbm, wk_hbm, wv_hbm)):
        for g in range(per):
            at = i * per + g
            load = pltpu.make_async_copy(
                hbm.at[:, g * group : (g + 1) * group], w_ref.at[at], semw.at[at]
            )
            load.start()
            loads.append(load)

    barrier = pltpu.get_barrier_semaphore()
    for k in range(1, n):
        pl.semaphore_signal(
            barrier, inc=1, device_id=(lax.rem(me + k, n), t), device_id_type=MESH
        )
    for k in range(1, m):
        pl.semaphore_signal(
            barrier, inc=1, device_id=(me, lax.rem(t + k, m)), device_id_type=MESH
        )
    pl.semaphore_wait(barrier, n + m - 2)

    first = []
    for k in range(1, n):
        peer = lax.rem(me + k, n)
        sems = (sem1.at[0, k], sem1.at[1, k])
        first.append(remote(inp_ref.at[peer], recv.at[me], sems, (peer, t)))
    recv[me] = inp_ref[me]
    for copy in first:
        copy.wait_recv()

    second = []
    for k in range(1, n):
        peer = lax.rem(me + k, n)
        send[k, :split] = recv[source_of(peer), :split]
        send[k, split:] = recv[task_at(peer), split:]
        sems = (sem2.at[0, k], sem2.at[1, k])
        second.append(remote(send.at[k], full.at[t, me], sems, (peer, t)))
    full[t, me, :split] = recv[source_of(me), :split]
    full[t, me, split:] = recv[task_at(me), split:]

    def hop(origin, k, distance, way):
        place = full.at[origin, lax.rem(me + n - k, n)]
        sems = (semz.at[0, way, distance, k], semz.at[1, way, distance, k])
        return remote(place, place, sems, (me, left if way else right))

    def reach(k, way):
        half = m // 2
        return half if way == k % 2 else m - 1 - half

    hops = {}
    for k in range(n):
        if k:
            second[k - 1].wait_recv()
        for way in (0, 1):
            hops[way, 1, k] = hop(t, k, 1, way)

    own = full[t].reshape(rows, width).astype(f32)
    square = jnp.sum(own * own, axis=1, keepdims=True)
    squares[0] = jnp.broadcast_to(square, (rows, 128)).T[:8]
    shared = []
    for k in range(1, m):
        peer = lax.rem(t + k, m)
        sems = (semq.at[0, k], semq.at[1, k])
        shared.append(remote(squares.at[0], squares.at[k], sems, (me, peer)))

    def origin_of(distance, way):
        return lax.rem(t + (m - distance if way == 0 else distance), m)

    def receive(distance):
        for k in range(n):
            for way in (0, 1):
                if distance <= reach(k, way):
                    hops[way, distance, k].wait_recv()
                    if distance < reach(k, way):
                        origin = origin_of(distance, way)
                        hops[way, distance + 1, k] = hop(origin, k, distance + 1, way)

    def project(origin, fresh):
        wide = full[origin].reshape(rows, width).astype(f32)
        normed = (wide * inv_ref[:, :1] * gain_ref[origin]).astype(bf16)
        deep = pl.ds(pl.multiple_of(origin * width, width), width)

        def body(b, carry):
            product = dot_nn(normed, w_ref[b, deep, :])
            qkv[b] = product if fresh else qkv[b] + product
            return carry

        lax.fori_loop(0, blocks, body, 0)

    receive(1)
    for copy in shared:
        copy.wait_recv()
    square = squares[0]
    for k in range(1, m):
        square = square + squares[k]
    square = jnp.broadcast_to(square[:1], (128, rows)).T
    inv_ref[...] = lax.rsqrt(square * (1.0 / model_width) + 1e-05)
    for load in loads:
        load.wait()
    project(t, True)
    project(origin_of(1, 0), False)
    project(origin_of(1, 1), False)
    for distance in range(2, m // 2 + 1):
        receive(distance)
        project(origin_of(distance, 0), False)
        if 2 * distance != m:
            project(origin_of(distance, 1), False)

    def prompt_rows(value):
        return value.reshape(n, chunk, value.shape[-1])[:, split:].reshape(
            n * lead, value.shape[-1]
        )

    limit = p_len + pick(me, lambda e: length_ref[e])
    scale = 1.0 / math.sqrt(HD)

    def heads(g, carry):
        cosine, sine = cos_ref[...], sin_ref[...]
        cosine_p, sine_p = prompt_rows(cosine), prompt_rows(sine)
        row_pos, col_pos = posr_ref[...], posc_ref[...]
        allowed = (col_pos <= row_pos) & (col_pos < limit)
        live = row_pos < limit
        for h in range(group // HD):
            at = slice(h * HD, (h + 1) * HD)
            far = pl.ds(pl.multiple_of(g * group + h * HD, HD), HD)
            q, k = qkv[g, :, at], qkv[per + g, :, at]
            v = qkv[2 * per + g, :, at].astype(bf16)
            q = (q * cosine + pltpu.roll(q, HD // 2, 1) * sine).astype(bf16)
            k = (k * cosine + pltpu.roll(k, HD // 2, 1) * sine).astype(bf16)
            scores = jnp.where(allowed, dot_nt(q, k) * scale, -1e30)
            peak = jnp.max(scores, axis=1, keepdims=True)
            weights = jnp.exp(scores - peak)
            probs = weights * (1.0 / jnp.sum(weights, axis=1, keepdims=True))
            low = probs.astype(bf16)
            out_ref[:, far] = jnp.where(live, dot_nn(low, v), 0.0).astype(bf16)
            upstream = jnp.where(live, cot_ref[:, far].astype(f32), 0.0).astype(bf16)
            grad_prob = dot_nt(upstream, v)
            delta = jnp.sum(probs * grad_prob, axis=1, keepdims=True)
            grad_score = probs * (grad_prob - delta)
            gq = dot_nn(prompt_rows(grad_score).astype(bf16), k) * scale
            gk = prompt_rows(dot_tn(grad_score.astype(bf16), q)) * scale
            gv = prompt_rows(dot_tn(low, upstream))
            gq = gq * cosine_p - pltpu.roll(gq, HD // 2, 1) * sine_p
            gk = gk * cosine_p - pltpu.roll(gk, HD // 2, 1) * sine_p
            grads[g, :, at] = gq.astype(bf16)
            grads[per + g, :, at] = gk.astype(bf16)
            grads[2 * per + g, :, at] = gv.astype(bf16)
        return carry

    lax.fori_loop(0, per, heads, 0)

    def prompts_of(z):
        return full[z, :, split:, :].astype(f32).reshape(n * lead, width)

    def back(z, dots):
        deep = pl.ds(pl.multiple_of(z * width, width), width)
        total = dot_nt(grads[0], w_ref[0, deep, :])
        for b in range(1, blocks):
            total = total + dot_nt(grads[b], w_ref[b, deep, :])
        total = total * gain_ref[z]
        acc[z] = total
        return dots + jnp.sum(total * prompts_of(z), axis=1, keepdims=True)

    dots = lax.fori_loop(0, m, back, jnp.zeros((n * lead, 1), f32))
    inv = prompt_rows(inv_ref[...])[:, :1]
    factor = inv * inv * inv * (dots * (1.0 / model_width))

    partial = {}
    for step in range(m):
        z = lax.rem(t + (2, 1, 3, 0)[step] if m == 4 else t + m - 1 - step, m)
        value = (inv * acc[z] - prompts_of(z) * factor).astype(bf16)
        part[z] = value.reshape(n, lead, width)
        if step < m - 1:
            for k in range(n):
                at = lax.rem(me + k, n)
                sems = (semg.at[0, step, k], semg.at[1, step, k])
                partial[step, k] = remote(
                    part.at[z, at], recvz.at[step, at], sems, (me, z), holds(at)
                )

    third = []
    for k in range(n):
        at = lax.rem(me + k, n)

        @pl.when(holds(at))
        def _():
            total = part[t, at].astype(f32)
            for step in range(m - 1):
                partial[step, k].wait_recv()
                total = total + recvz[step, at].astype(f32)
            if k == 0:
                recv1[me] = total.astype(bf16)
            else:
                send1[k] = total.astype(bf16)

        if k:
            sems = (sem3.at[0, k], sem3.at[1, k])
            third.append(remote(send1.at[k], recv1.at[me], sems, (at, t), holds(at)))

    @pl.when(holds(me))
    def _():
        for copy in third:
            copy.wait_recv()

    tasks = [task_at(s) for s in range(n)]
    fourth = []
    for k in range(n):
        peer = lax.rem(me + k, n)

        @pl.when(holds(me))
        def _():
            total = jnp.zeros((lead, width), f32)
            for s in range(n):
                hit = jnp.where(tasks[s] == peer, 1.0, 0.0)
                total = total + hit * recv1[s].astype(f32)
            if k == 0:
                recv2[me] = total.astype(bf16)
            else:
                send2[k] = total.astype(bf16)

        if k:
            sems = (sem4.at[0, k], sem4.at[1, k])
            fourth.append(remote(send2.at[k], recv2.at[me], sems, (peer, t), holds(me)))
    for k in range(1, n):
        pl.when(holds(lax.rem(me + n - k, n)))(fourth[k - 1].wait_recv)
    for at in range(n):
        if at * lead < p_len:
            grad_ref[at] = recv2[at].astype(f32)
        else:
            grad_ref[at] = jnp.zeros((lead, width), f32)
    for copy in first + second + list(hops.values()) + shared:
        copy.wait_send()
    for (_, k), copy in partial.items():
        pl.when(holds(lax.rem(me + k, n)))(copy.wait_send)
    for k in range(1, n):
        pl.when(holds(lax.rem(me + k, n)))(third[k - 1].wait_send)
        pl.when(holds(me))(fourth[k - 1].wait_send)


def fast_device(text, prompts, gain, w_query, w_key, w_value, cotangent, task_of, lengths, slot):
    n, m = lax.axis_size("dp"), lax.axis_size("tensor")
    f32, bf16 = jnp.float32, jnp.bfloat16
    seq, width = text.shape[1], text.shape[2]
    p_len = prompts.shape[1]
    ct = seq // n
    cp = ct // 2
    chunk = ct + cp
    rows = n * chunk
    heads = w_query.shape[1]

    def interleave(tail, lead):
        lead = jnp.pad(lead, ((0, n * cp - p_len), (0, 0)))
        parts = [tail.reshape(n, ct, -1), lead.reshape(n, cp, -1)]
        return jnp.concatenate(parts, axis=1)

    row = np.arange(rows, dtype=np.int32)
    j, i = row // chunk, row % chunk
    lead_pos = j * cp + i - ct
    lead_pos = np.where(lead_pos < p_len, lead_pos, PAD_POS)
    pos = np.where(i < ct, p_len + j * ct + i, lead_pos).astype(np.int32)
    half = HD // 2
    frequency = 10000.0 ** (-jnp.arange(half, dtype=f32) / half)
    angle = jnp.asarray(np.where(pos < PAD_POS, pos, 0)).astype(f32)[:, None] * frequency[None, :]
    cosine = jnp.concatenate([jnp.cos(angle)] * 2, axis=1)
    sine = jnp.concatenate([-jnp.sin(angle), jnp.sin(angle)], axis=1)
    cot = interleave(cotangent[0, p_len:], cotangent[0, :p_len]).reshape(rows, heads)
    group = 2 * HD if heads % (2 * HD) == 0 else HD
    blocks = 3 * (heads // group)
    smem = pl.BlockSpec(memory_space=pltpu.SMEM)
    vmem = pl.BlockSpec(memory_space=pltpu.VMEM)
    hbm = pl.BlockSpec(memory_space=pl.ANY)
    dma = pltpu.SemaphoreType.DMA
    out, collected = pl.pallas_call(
        functools.partial(step_kernel, p_len),
        out_shape=(
            jax.ShapeDtypeStruct((rows, heads), bf16),
            jax.ShapeDtypeStruct((n, cp, width), f32),
        ),
        in_specs=[smem] * 3 + [vmem] * 7 + [hbm] * 3,
        out_specs=(vmem, vmem),
        scratch_shapes=[
            pltpu.VMEM((blocks, m * width, group), bf16),
            pltpu.VMEM((n, chunk, width), bf16),
            pltpu.VMEM((n, chunk, width), bf16),
            pltpu.VMEM((m, n, chunk, width), bf16),
            pltpu.VMEM((m, 8, rows), f32),
            pltpu.VMEM((blocks, rows, group), f32),
            pltpu.VMEM((blocks, n * cp, group), bf16),
            pltpu.VMEM((rows, 128), f32),
            pltpu.VMEM((m, n * cp, width), f32),
            pltpu.VMEM((m, n, cp, width), bf16),
            pltpu.VMEM((m - 1, n, cp, width), bf16),
            pltpu.VMEM((n, cp, width), bf16),
            pltpu.VMEM((n, cp, width), bf16),
            pltpu.VMEM((n, cp, width), bf16),
            pltpu.VMEM((n, cp, width), bf16),
            dma((blocks,)),
            dma((2, n)),
            dma((2, n)),
            dma((2, 2, m // 2 + 1, n)),
            dma((2, m)),
            dma((2, m, n)),
            dma((2, n)),
            dma((2, n)),
        ],
        compiler_params=pltpu.CompilerParams(
            collective_id=0, has_side_effects=True, vmem_limit_bytes=63 * 2**20
        ),
    )(
        slot, task_of, lengths, interleave(text[0], prompts[0]), gain.reshape(m, 1, width),
        cosine, sine, jnp.asarray(pos[:, None]), jnp.asarray(pos[None, :]), cot, w_query, w_key, w_value,
    )
    prompt_grad = collected.reshape(n * cp, width)[:p_len][None]
    out = out.reshape(n, chunk, heads)
    lead = out[:, ct:].reshape(n * cp, heads)[:p_len]
    attn_out = jnp.concatenate([lead, out[:, :ct].reshape(seq, heads)], axis=0)[None]
    return (attn_out, prompt_grad)


def choose(text, prompts, *rest):
    n, m = lax.axis_size("dp"), lax.axis_size("tensor")
    seq, p_len = text.shape[1], prompts.shape[1]
    fits = (
        text.shape[0] == 1
        and prompts.shape[0] == 1
        and m >= 3
        and n >= 2
        and seq % (32 * n) == 0
        and p_len <= seq // 2
        and text.shape[2] % 128 == 0
    )
    return (fast_device if fits else on_device)(text, prompts, *rest)


def solution(mesh):
    in_specs = (
        P("dp", None, "tensor"),
        P("dp", None, "tensor"),
        P(),
        P(None, "tensor"),
        P(None, "tensor"),
        P(None, "tensor"),
        P("dp", None, "tensor"),
        P(),
        P(),
        P(),
    )
    out_specs = (P("dp", None, "tensor"), P("dp", None, "tensor"))
    return jax.shard_map(
        choose, mesh=mesh, in_specs=in_specs, out_specs=out_specs, check_vma=False
    )
```
